256 devices in a mesh: dp: 32 (over y, z), tensor: 8 (over x, core).
Axes of the slice: x: 4, y: 4, z: 8, core: 2. Of those that a mesh axis runs over, the one named last changes fastest.
Arguments:
- hidden: bfloat16 [8192, 18432], P('dp', 'tensor'), may hold values from -6 to 6
- down_weight: bfloat16 [18432, 4608], P('tensor', 'dp'), may hold values from -0.046875 to 0.046875
- residual: bfloat16 [8192, 4608], P('dp'), may hold values from -6 to 6
- post_gain: float32 [4608], replicated, may hold values from 0.5 to 1.5
- pre_gain: float32 [4608], replicated, may hold values from 0.5 to 1.5
- cast_scale: float32 [1], replicated, may hold values from 100 to 400
- amax_history: float32 [3, 1024], replicated, may hold values from 0.25 to 4
Outputs:
- cast_out: bfloat16 [8192, 4608], P('dp')
- residual_out: bfloat16 [8192, 4608], P('dp')
- peaks: float32 [3], replicated
- new_history: float32 [3, 1024], replicated
- new_scales: float32 [3], replicated
The draws below stay inside these ranges and needn't reach their ends.
All inputs are finite; a program needn't handle non-finite values.
Results may differ from the reference program's by a relative error of at most 0.012.
Values may be sent and summed in bfloat16 or wider, within the bound.
No kernel may reach another device: no remote copies, remote signals or barrier semaphores. Data moves between devices by JAX's collectives and lax.ppermute only.
A program may use at most 128 MiB of HBM per device.

```python
import math
import jax
import jax.numpy as jnp
from jax import lax

D = 4608
FF_WIN = 18432
HIST = 1024
FF_DEV = 2304
TOKENS = 8192


def block_scale(key, shape, split, low, top_value):
    gain, own = 1.0, jax.random.fold_in(key, 6)
    for dim, shards_of in split:
        heights = jnp.exp(jax.random.uniform(jax.random.fold_in(own, dim), (shards_of,), jnp.float32, low / len(split), top_value / len(split)))
        gain = gain * jnp.repeat(heights, shape[dim] // shards_of).reshape([-1 if axis == dim else 1 for axis in range(len(shape))])
    return gain


def centred(own_key, dims, scale, most, pieces=(), kind=jnp.bfloat16):
    loudness = block_scale(own_key, dims, pieces, -0.22, 0.18) if pieces else 1.0
    array = jax.random.normal(own_key, dims, jnp.float32) * scale * loudness
    return jnp.minimum(jnp.maximum(array, -most), most).astype(kind)


def setup_inputs(seed: int = 0) -> dict:
    key_list = jax.random.split(jax.random.key(seed), 8)
    hidden = centred(key_list[0], (TOKENS, FF_WIN), 1.0, 6.0, ((0, 32), (1, 8)))
    down_weight = centred(key_list[1], (FF_WIN, D), FF_WIN ** -0.5, 0.046875, ((0, 8), (1, 32)))
    residual = centred(key_list[2], (TOKENS, D), 1.0, 6.0, ((0, 32),))
    post_gain = jnp.clip(1.0 + 0.1 * jax.random.normal(key_list[3], (D,), jnp.float32), 0.5, 1.5)
    pre_gain = jnp.clip(1.0 + 0.1 * jax.random.normal(key_list[4], (D,), jnp.float32), 0.5, 1.5)
    cast_scale = jnp.clip(jnp.exp(jax.random.uniform(key_list[5], (1,), jnp.float32, math.log(100.0), math.log(400.0))), 100.0, 400.0)
    amax_history = jnp.clip(jnp.exp(jax.random.uniform(key_list[6], (3, HIST), jnp.float32, math.log(0.25), math.log(4.0))), 0.25, 4.0)
    return dict(hidden=hidden, down_weight=down_weight, residual=residual, post_gain=post_gain, pre_gain=pre_gain, cast_scale=cast_scale, amax_history=amax_history)


norm_epsilon = 1e-06
float_limit = 448.0

def rms_norm(values, gain_vector):
    return values * lax.rsqrt(lax.optimization_barrier(jnp.mean(values * values, axis=-1, keepdims=True)) + norm_epsilon) * gain_vector

def reference(hidden, down_weight, residual, post_gain, pre_gain, cast_scale, amax_history):
    summed = jnp.zeros((hidden.shape[0], down_weight.shape[1]), jnp.float32)
    for shard_index in range(FF_WIN // FF_DEV):
        first = shard_index * FF_DEV
        term = jnp.dot(hidden[:, first:first + FF_DEV], down_weight[first:first + FF_DEV, :], preferred_element_type=jnp.float32)
        term = lax.optimization_barrier(term.astype(jnp.bfloat16)).astype(jnp.float32)
        summed = summed + term
    stream = residual.astype(jnp.float32) + rms_norm(summed, post_gain)
    normed = rms_norm(stream, pre_gain)
    stale_scale = cast_scale[0]
    cast_out = (jnp.clip(normed * stale_scale, -float_limit, float_limit) / stale_scale).astype(jnp.bfloat16)
    peak_values = jnp.stack([jnp.max(jnp.abs(summed)), jnp.max(jnp.abs(stream)), jnp.max(jnp.abs(normed))]).astype(jnp.float32)
    new_history = jnp.concatenate([peak_values[:, None], amax_history[:, :-1]], axis=1)
    new_scales = float_limit / jnp.maximum(lax.optimization_barrier(jnp.max(new_history, axis=1)), 1.0)
    return (cast_out, stream.astype(jnp.bfloat16), peak_values, new_history, new_scales)
```

```python
import functools

import jax
import jax.numpy as jnp
from jax import lax
from jax.experimental import pallas as pl
from jax.experimental.pallas import tpu as pltpu
from jax.sharding import Mesh
from jax.sharding import PartitionSpec as P


DP = ("y", "z")
TENSOR = ("x", "c")

norm_epsilon = 1e-06
float_limit = 448.0

D = 4608
K = 2304
SHARD = 144
ROWS = 32
VMEM = pl.BlockSpec(memory_space=pltpu.VMEM)
SMEM = pl.BlockSpec(memory_space=pltpu.SMEM)


def call(body, ins, outs, scratch=(), name=None):
    return pl.pallas_call(
        body,
        in_specs=list(ins),
        out_specs=[VMEM] * len(outs),
        out_shape=outs,
        scratch_shapes=list(scratch),
        name=name,
        compiler_params=pltpu.CompilerParams(vmem_limit_bytes=56 * 2**20),
    )


def shape(dims, kind=jnp.bfloat16):
    return jax.ShapeDtypeStruct(dims, kind)


def shift(array, axis, by):
    n = lax.axis_size(axis)
    return lax.ppermute(array, axis, [(i, (i + by) % n) for i in range(n)])


def order_tokens(at, h0, h1, h2a, h2b, h3, out):
    for dc in range(2):
        for dx in range(4):
            t = lax.rem(at[0] + dx, 4) * 2 + (at[1] + dc) % 2
            rows = pl.ds(pl.multiple_of(t * ROWS, ROWS), ROWS)
            b = dc * 4 + dx
            out[b, pl.ds(0, ROWS), :] = h0[rows, :]
            out[b, pl.ds(ROWS, ROWS), :] = h1[rows, :]
            out[b, pl.ds(3 * ROWS, ROWS), :] = h3[rows, :]
            low = lax.rem(at[0] + dx, 4) < 2
            half = lax.rem(t, 4)
            there = pl.ds(pl.multiple_of(half * ROWS, ROWS), ROWS)

            @pl.when(low)
            def _():
                out[b, pl.ds(2 * ROWS, ROWS), :] = h2a[there, :]

            @pl.when(jnp.logical_not(low))
            def _():
                out[b, pl.ds(2 * ROWS, ROWS), :] = h2b[there, :]


def project(*refs):
    tokens, *shards, keep, send, weights = refs
    at = 0
    for shard in shards:
        weights[pl.ds(at, shard.shape[0]), :] = shard[...]
        at += shard.shape[0]
    for first in range(0, 8, 2):
        block = tokens[pl.ds(first, 2), :, :].reshape(256, K)
        term = lax.dot_general(
            weights[...], block, (((1,), (1,)), ((), ())), preferred_element_type=jnp.float32
        ).astype(jnp.bfloat16)
        out = keep if first < 4 else send
        out[first % 4] = term[:, :128]
        out[first % 4 + 1] = term[:, 128:]


def add_pair(keep, other, own, s1, s2, s3):
    own[...] = keep[0].astype(jnp.float32) + other[0].astype(jnp.float32)
    for dx, out in ((1, s1), (2, s2), (3, s3)):
        out[...] = (keep[dx].astype(jnp.float32) + other[dx].astype(jnp.float32)).astype(
            jnp.bfloat16
        )


def own_rows_of(at, a0, a1, a2, a3, b0, b1, b2, b3, o0, o1, o2, o3, columns):
    for blocks, dists in (((a0, a1, a2, a3), (-2, -1, 0, 1, 2)), ((b0, b1, b2, b3), (3, 4, 5))):
        for i, dist in enumerate(dists):
            rows = pl.ds(i * SHARD, SHARD)
            total = blocks[0][rows, :]
            for block in blocks[1:]:
                total = total + block[rows, :].astype(jnp.float32)
            place = lax.rem(at[3] + (dist + 8), 8) * SHARD
            columns[pl.ds(pl.multiple_of(place, SHARD), SHARD), :] = total
    whole = columns[...].T.astype(jnp.bfloat16)
    for d, out in enumerate((o0, o1, o2, o3)):
        out[...] = whole[d * ROWS : (d + 1) * ROWS, :]


def rms(values, gain_vector):
    return (
        values
        * lax.rsqrt(jnp.mean(values * values, axis=-1, keepdims=True) + norm_epsilon)
        * gain_vector
    )


def finish(at, r0, r1, r2, r3, residual, post_gain, pre_gain, stream_out, peaks, summed):
    for d, block in enumerate((r0, r1, r2, r3)):
        place = lax.rem(at[2] + (4 - d), 4) * 1152
        summed[:, pl.ds(pl.multiple_of(place, 1152), 1152)] = block[...].astype(jnp.float32)
    t = at[0] * 2 + at[1]
    total = summed[...]
    own = residual[pl.ds(pl.multiple_of(t * ROWS, ROWS), ROWS), :]
    stream = own.astype(jnp.float32) + rms(total, post_gain[...])
    stream_out[...] = stream.astype(jnp.bfloat16)
    normed = rms(stream, pre_gain[...])
    most = [
        jnp.max(jnp.abs(v), axis=(0, 1), keepdims=True) for v in (total, stream, normed)
    ]
    row = lax.broadcasted_iota(jnp.int32, (8, 128), 0)
    peaks[...] = jnp.where(row == 0, most[0], jnp.where(row == 1, most[1], most[2]))


def cast_rows(at, scale, pre_gain, *refs):
    blocks, (cast_out, residual_out) = refs[:8], refs[8:]
    s = scale[0]
    back = 1.0 / jnp.full((1, 1), s, jnp.float32)
    for dc in range(2):
        for dx in range(4):
            t = lax.rem(at[0] + (4 - dx), 4) * 2 + (at[1] + dc) % 2
            rows = pl.ds(pl.multiple_of(t * ROWS, ROWS), ROWS)
            rounded = blocks[dc * 4 + dx][...]
            residual_out[rows, :] = rounded
            normed = rms(rounded.astype(jnp.float32), pre_gain[...])
            cast_out[rows, :] = (jnp.clip(normed * s, -float_limit, float_limit) * back).astype(
                jnp.bfloat16
            )


def on_device(hidden, down_weight, residual, post_gain, pre_gain, cast_scale, amax_history):
    at = jnp.stack([lax.axis_index(a) for a in ("x", "c", "y", "z")]).astype(jnp.int32)
    w0 = down_weight.T

    wr1, wl1 = shift(w0, "z", 1), shift(w0, "z", -1)
    hr1, hl1 = shift(hidden, "y", 1), shift(hidden, "y", -1)
    wr2, wl2 = shift(wr1, "z", 1), shift(wl1, "z", -1)
    h2a, h2b = shift(hr1[:128], "y", 1), shift(hl1[128:], "y", -1)
    wr3, wl3 = shift(wr2, "z", 1), shift(wl2, "z", -1)
    wr4, wl4 = shift(wr3[:80], "z", 1), shift(wl3[80:], "z", -1)

    (tokens,) = call(
        order_tokens, [SMEM] + [VMEM] * 5, [shape((8, 128, K))], name="order_tokens"
    )(at, hidden, hl1, h2a, h2b, hr1)

    def partial_sums(shards, width):
        blocks = shape((4, width, 128))
        keep, send = call(
            project,
            [VMEM] * (1 + len(shards)),
            [blocks, blocks],
            [pltpu.VMEM((width, K), jnp.bfloat16)],
            name="project",
        )(tokens, *shards)
        other = shift(send, "c", 1)
        own, s1, s2, s3 = call(
            add_pair,
            [VMEM] * 2,
            [shape((width, 128), jnp.float32)] + [shape((width, 128))] * 3,
            name="add_pair",
        )(keep, other)
        return own, shift(s1, "x", 1), shift(s2, "x", 2), shift(s3, "x", 3)

    near = partial_sums((wr2, wr1, w0, wl1, wl2), 720)
    far = partial_sums((wl3, wr4, wl4, wr3), 432)

    o0, o1, o2, o3 = call(
        own_rows_of,
        [SMEM] + [VMEM] * 8,
        [shape((ROWS, 1152))] * 4,
        [pltpu.VMEM((1152, 128), jnp.float32)],
        name="own_rows_of",
    )(at, *near, *far)
    r1, r2, r3 = shift(o1, "y", 1), shift(o2, "y", 2), shift(o3, "y", 3)

    stream, peaks = call(
        finish,
        [SMEM] + [VMEM] * 7,
        [shape((ROWS, D)), shape((8, 128), jnp.float32)],
        [pltpu.VMEM((ROWS, D), jnp.float32)],
        name="finish",
    )(at, o0, r1, r2, r3, residual, post_gain[None], pre_gain[None])

    mine = [stream] + [shift(stream, "x", d) for d in (1, 2, 3)]
    partners = [shift(b, "c", 1) for b in mine]

    for axis in ("y", "z", "c", "x"):
        others = [shift(peaks, axis, d) for d in range(1, lax.axis_size(axis))]
        peaks = functools.reduce(jnp.maximum, others, peaks)

    cast_out, residual_out = call(
        cast_rows,
        [SMEM, SMEM] + [VMEM] * 9,
        [shape((256, D)), shape((256, D))],
        name="cast_rows",
    )(at, cast_scale, pre_gain[None], *mine, *partners)

    peak_values = peaks[:3, 0]
    new_history = jnp.concatenate([peak_values[:, None], amax_history[:, :-1]], axis=1)
    new_scales = float_limit / jnp.maximum(jnp.max(new_history, axis=1), 1.0)
    return (cast_out, residual_out, peak_values, new_history, new_scales)


def solution(mesh):
    split = Mesh(mesh.devices.reshape(4, 8, 4, 2), ("y", "z", "x", "c"))
    in_specs = (P(DP, TENSOR), P(TENSOR, DP), P(DP, None), P(), P(), P(), P())
    out_specs = (P(DP, None), P(DP, None), P(), P(), P())
    return jax.shard_map(
        on_device, mesh=split, in_specs=in_specs, out_specs=out_specs, check_vma=False
    )
```

```python
import functools

import jax
import jax.numpy as jnp
from jax import lax
from jax.experimental import pallas as pl
from jax.experimental.pallas import tpu as pltpu
from jax.sharding import Mesh
from jax.sharding import PartitionSpec as P


DP = ("y", "z")
TENSOR = ("x", "c")

norm_epsilon = 1e-06
float_limit = 448.0

D = 4608
K = 2304
SHARD = 144
ROWS = 32
NEAR = 768
FAR = 512
VMEM = pl.BlockSpec(memory_space=pltpu.VMEM)
ANY = pl.BlockSpec(memory_space=pl.ANY)
SMEM = pl.BlockSpec(memory_space=pltpu.SMEM)


def call(body, ins, outs, scratch=(), mib=4, out=VMEM, aliases={}):
    return pl.pallas_call(
        body,
        in_specs=list(ins),
        out_specs=[out] * len(outs),
        out_shape=outs,
        scratch_shapes=list(scratch),
        input_output_aliases=aliases,
        compiler_params=pltpu.CompilerParams(vmem_limit_bytes=mib * 2**20),
    )


def shape(dims, kind=jnp.bfloat16):
    return jax.ShapeDtypeStruct(dims, kind)


def shift(array, axis, by):
    n = lax.axis_size(axis)
    return lax.ppermute(array, axis, [(i, (i + by) % n) for i in range(n)])


def owner_rows(at, dc, dx):
    t = lax.rem(at[0] + dx, 4) * 2 + (at[1] + dc) % 2
    return pl.ds(pl.multiple_of(t * ROWS, ROWS), ROWS)


def stack(weights, at, shards):
    for shard in shards:
        weights[pl.ds(at, shard.shape[0]), :] = shard[...]
        at += shard.shape[0]


BLOCKS = tuple((dc * 4 + dx, dc, dx) for dc in range(2) for dx in range(4))


def prepare(at, h0, a0, b0, tokens, weights, sems):
    copies = [
        pltpu.make_async_copy(
            h0.at[owner_rows(at, dc, dx), :], tokens.at[b, pl.ds(0, ROWS), :], sems.at[b]
        )
        for b, dc, dx in BLOCKS
    ]
    for copy in copies:
        copy.start()
    stack(weights, 2 * SHARD, (a0, b0))
    for copy in copies:
        copy.wait()


def halve(h1, h3, high, low):
    high[...] = h1[128:, :]
    low[...] = h3[:128, :]


def order_first(at, h1, h3, _, tokens):
    for b, dc, dx in BLOCKS:
        for i, h in ((1, h1), (2, h3)):
            tokens[b, pl.ds(i * ROWS, ROWS), :] = h[owner_rows(at, dc, dx), :]


def order_last(at, h2a, h2b, out):
    for dc in range(2):
        for dx in range(4):
            x = lax.rem(at[0] + dx, 4)
            t = x * 2 + (at[1] + dc) % 2
            rows = pl.ds(pl.multiple_of(lax.rem(t, 4) * ROWS, ROWS), ROWS)

            @pl.when(x < 2)
            def _():
                out[dc * 4 + dx] = h2a[rows, :]

            @pl.when(x >= 2)
            def _():
                out[dc * 4 + dx] = h2b[rows, :]


def lanes_of(j):
    return slice(None) if j is None else pl.ds(pl.multiple_of(j * 256, 256), 256)


def times(tokens, weights, j):
    blocks, rows, _ = tokens.shape
    return (
        lax.dot_general(
            tokens[...].reshape(blocks * rows, K),
            weights[lanes_of(j), :],
            (((1,), (1,)), ((), ())),
            preferred_element_type=jnp.float32,
        )
        .astype(jnp.bfloat16)
        .reshape(blocks, rows, -1)
    )


def store_first(terms, keep, send, j):
    for out, b in ((keep, 0), (send, 4)):
        out[:, pl.ds(0, 2 * ROWS), lanes_of(j)] = terms[b : b + 4, : 2 * ROWS]
        out[:, pl.ds(3 * ROWS, ROWS), lanes_of(j)] = terms[b : b + 4, 2 * ROWS :]


def store_last(terms, keep, send, j):
    for out, b in ((keep, 0), (send, 4)):
        out[:, pl.ds(2 * ROWS, ROWS), lanes_of(j)] = terms[b : b + 4]


def project_first(tokens, *refs):
    *shards, _, out, weights = refs
    stack(weights, 0, shards[:4])
    stack(weights, 3 * SHARD, shards[4:])

    def tile(j, _):
        out[:, :, lanes_of(j)] = times(tokens, weights, j)

    lax.fori_loop(0, NEAR // 256, tile, None)


def project_last(tokens, weights, done, keep, send):
    store_last(times(tokens, weights, None), keep, send, None)
    store_first(done[...], keep, send, None)


def stack_far(l3a, l3b, r3a, r3b, weights):
    stack(weights, 80, (l3a, l3b))
    stack(weights, 80 + 2 * SHARD, (r3a, r3b))


def project_far(first, last, r4a, l4b, _, keep, send, weights):
    stack(weights, 80 + SHARD, (r4a, l4b))

    def tile(j, _):
        store_first(times(first, weights, j), keep, send, j)
        store_last(times(last, weights, j), keep, send, j)

    lax.fori_loop(0, FAR // 256, tile, None)


def pair_sum(keep, other, dx):
    return keep[dx].astype(jnp.float32) + other[dx].astype(jnp.float32)


def add_pair(keep, other, own, s1, s2, s3):
    own[...] = pair_sum(keep, other, 0)
    for dx, out in ((1, s1), (2, s2), (3, s3)):
        out[...] = pair_sum(keep, other, dx).astype(jnp.bfloat16)


def own_rows_of(at, n0, n1, n2, n3, f0, f1, f2, f3, o0, o1, o2, o3, columns):
    def total(parts, lanes):
        return functools.reduce(jnp.add, [p[:, lanes].astype(jnp.float32) for p in parts])

    near_sum = functools.partial(total, (n0, n1, n2, n3))
    far_sum = functools.partial(total, (f0, f1, f2, f3))
    columns[:, :640] = near_sum(slice(0, 640))
    lane = lax.broadcasted_iota(jnp.int32, (128, 128), 1)
    columns[:, 640:768] = jnp.where(
        lane < 80, near_sum(slice(640, 768)), far_sum(slice(0, 128))
    )
    columns[:, 768:] = far_sum(slice(128, 512))
    turn = lax.rem(at[3] + 6, 8) * SHARD
    whole = pltpu.roll(columns[...], turn, 1).astype(jnp.bfloat16)
    for d, out in enumerate((o0, o1, o2, o3)):
        out[...] = whole[d * ROWS : (d + 1) * ROWS, :]


def rms(values, gain_vector):
    return (
        values
        * lax.rsqrt(jnp.mean(values * values, axis=-1, keepdims=True) + norm_epsilon)
        * gain_vector
    )


def finish(at, r0, r1, r2, r3, residual, post_gain, pre_gain, stream_out, peaks, summed):
    for d, block in enumerate((r0, r1, r2, r3)):
        place = lax.rem(at[2] + (4 - d), 4) * 1152
        summed[:, pl.ds(pl.multiple_of(place, 1152), 1152)] = block[...].astype(jnp.float32)
    t = at[0] * 2 + at[1]
    total = summed[...]
    own = residual[pl.ds(pl.multiple_of(t * ROWS, ROWS), ROWS), :]
    stream = own.astype(jnp.float32) + rms(total, post_gain[...])
    rounded = stream.astype(jnp.bfloat16)
    for i in range(4):
        stream_out[i] = rounded
    normed = rms(stream, pre_gain[...])
    most = [
        jnp.max(jnp.abs(v), axis=(0, 1), keepdims=True) for v in (total, stream, normed)
    ]
    column = lax.broadcasted_iota(jnp.int32, (8, 128), 1)
    peaks[...] = jnp.where(column == 0, most[0], jnp.where(column == 1, most[1], most[2]))


def cast_rows(dc, at, scale, pre_gain, blocks, *refs):
    cast_out, residual_out, cast, sems = refs[-4:]
    s = scale[0]
    back = 1.0 / jnp.full((1, 1), s, jnp.float32)

    def copies(x):
        t = 2 * x + (at[1] + dc) % 2
        rows = pl.ds(pl.multiple_of(t * ROWS, ROWS), ROWS)
        return (
            pltpu.make_async_copy(blocks.at[x], residual_out.at[rows, :], sems.at[0, x]),
            pltpu.make_async_copy(cast.at[x], cast_out.at[rows, :], sems.at[1, x]),
        )

    def start(x, _):
        from_blocks, from_cast = copies(x)
        from_blocks.start()
        normed = rms(blocks[x].astype(jnp.float32), pre_gain[...])
        cast[x] = (jnp.clip(normed * s, -float_limit, float_limit) * back).astype(jnp.bfloat16)
        from_cast.start()

    lax.fori_loop(0, 4, start, None)
    for x in range(4):
        for copy in copies(x):
            copy.wait()


def cast(scaled, blocks, dc, halves):
    return call(
        functools.partial(cast_rows, dc),
        [SMEM, SMEM] + [VMEM] * 2 + [ANY] * (2 if halves else 0),
        [shape((256, D)), shape((256, D))],
        [pltpu.VMEM((4, ROWS, D), jnp.bfloat16), pltpu.SemaphoreType.DMA((2, 4))],
        mib=6,
        out=ANY,
        aliases={4: 0, 5: 1} if halves else {},
    )(*scaled, blocks, *(halves or ()))


def sums_along_x(keep, send):
    other = shift(send, "c", 1)
    width = keep.shape[2]
    own, *others = call(
        add_pair, [VMEM] * 2, [shape((128, width), jnp.float32)] + [shape((128, width))] * 3
    )(keep, other)
    return own, *(shift(s, "x", d) for d, s in enumerate(others, 1))


def on_device(hidden, down_weight, residual, post_gain, pre_gain, cast_scale, amax_history):
    at = jnp.stack([lax.axis_index(a) for a in ("x", "c", "y", "z")]).astype(jnp.int32)
    shards = down_weight.T
    a0, b0 = shards[:80], shards[80:]

    right, left = {0: (a0, b0)}, {0: (a0, b0)}
    for step in (1, 2, 3):
        ar = shift(right[step - 1][0], "z", 1)
        al = shift(left[step - 1][0], "z", -1)
        br = shift(right[step - 1][1], "z", 1)
        bl = shift(left[step - 1][1], "z", -1)
        right[step], left[step] = (ar, br), (al, bl)
    w4 = (shift(right[3][0], "z", 1), shift(left[3][1], "z", -1))

    h3, h1 = shift(hidden, "y", 1), shift(hidden, "y", -1)
    high, low = call(halve, [VMEM] * 2, [shape((128, K))] * 2, mib=5)(h1, h3)
    h2a, h2b = shift(low, "y", 1), shift(high, "y", -1)

    tokens, near_weights = call(
        prepare,
        [SMEM, ANY] + [VMEM] * 2,
        [shape((8, 96, K)), shape((NEAR, K))],
        [pltpu.SemaphoreType.DMA((8,))],
        mib=9,
    )(at, hidden, a0, b0)
    (first,) = call(
        order_first, [SMEM] + [VMEM] * 3, [shape((8, 96, K))], mib=10, aliases={3: 0}
    )(at, h1, h3, tokens)
    (last,) = call(order_last, [SMEM] + [VMEM] * 2, [shape((8, ROWS, K))], mib=4)(at, h2a, h2b)

    near_shards = (*right[2], *right[1], *left[1], *left[2])
    near, near_weights = call(
        project_first,
        [VMEM] * (2 + len(near_shards)),
        [shape((8, 96, NEAR)), shape((NEAR, K))],
        aliases={9: 1},
        mib=14,
    )(first, *near_shards, near_weights)
    keep, send = call(
        project_last, [VMEM] * 3, [shape((4, 128, NEAR))] * 2, mib=9
    )(last, near_weights, near)
    near_parts = sums_along_x(keep, send)

    (far_weights,) = call(stack_far, [VMEM] * 4, [shape((FAR, K))], mib=5)(*left[3], *right[3])
    keep, send, _ = call(
        project_far,
        [VMEM] * 5,
        [shape((4, 128, FAR))] * 2 + [shape((FAR, K))],
        aliases={4: 2},
        mib=13,
    )(first, last, *w4, far_weights)
    far_parts = sums_along_x(keep, send)

    o0, o1, o2, o3 = call(
        own_rows_of,
        [SMEM] + [VMEM] * 8,
        [shape((ROWS, 1152))] * 4,
        [pltpu.VMEM((128, 1152), jnp.float32)],
    )(at, *near_parts, *far_parts)
    r1, r2, r3 = (shift(o, "y", d) for d, o in ((1, o1), (2, o2), (3, o3)))

    stream, peaks = call(
        finish,
        [SMEM] + [VMEM] * 7,
        [shape((4, ROWS, D)), shape((8, 128), jnp.float32)],
        [pltpu.VMEM((ROWS, D), jnp.float32)],
        mib=8,
    )(at, o0, r1, r2, r3, residual, post_gain[None], pre_gain[None])

    mine = lax.all_to_all(stream, "x", 0, 0, tiled=True)
    partners = shift(mine, "c", 1)

    def most_along(peaks, axis, steps):
        others = [shift(peaks, axis, d) for d in steps]
        return functools.reduce(jnp.maximum, others, peaks)

    for axis, steps in (("x", (1, 2, 3)), ("c", (1,)), ("y", (1, 2, 3)), ("z", (1, 7)), ("z", (3, 5))):
        peaks = most_along(peaks, axis, steps)
    peak_values = peaks[0, :3]

    scaled = (at, cast_scale, pre_gain[None])
    halves = cast(scaled, mine, 0, None)
    cast_out, residual_out = cast(scaled, partners, 1, halves)

    new_history = jnp.concatenate([peak_values[:, None], amax_history[:, :-1]], axis=1)
    new_scales = float_limit / jnp.maximum(jnp.max(new_history, axis=1), 1.0)
    return (cast_out, residual_out, peak_values, new_history, new_scales)


def solution(mesh):
    split = Mesh(mesh.devices.reshape(4, 8, 4, 2), ("y", "z", "x", "c"))
    in_specs = (P(DP, TENSOR), P(TENSOR, DP), P(DP, None), P(), P(), P(), P())
    out_specs = (P(DP, None), P(DP, None), P(), P(), P())

    return jax.shard_map(
        on_device, mesh=split, in_specs=in_specs, out_specs=out_specs, check_vma=False
    )
```

```python
import functools

import jax
import jax.numpy as jnp
from jax import lax
from jax.experimental import pallas as pl
from jax.experimental.pallas import tpu as pltpu
from jax.sharding import Mesh
from jax.sharding import PartitionSpec as P


DP = ("y", "z")
TENSOR = ("x", "c")

norm_epsilon = 1e-06
float_limit = 448.0

D = 4608
K = 2304
SHARD = 144
ROWS = 32
NEAR = 768
FAR = 512
VMEM = pl.BlockSpec(memory_space=pltpu.VMEM)
ANY = pl.BlockSpec(memory_space=pl.ANY)
SMEM = pl.BlockSpec(memory_space=pltpu.SMEM)


def call(body, ins, outs, scratch=(), mib=4, out=VMEM, aliases={}):
    return pl.pallas_call(
        body,
        in_specs=list(ins),
        out_specs=[out] * len(outs),
        out_shape=outs,
        scratch_shapes=list(scratch),
        input_output_aliases=aliases,
        compiler_params=pltpu.CompilerParams(vmem_limit_bytes=mib * 2**20),
    )


def shape(dims, kind=jnp.bfloat16):
    return jax.ShapeDtypeStruct(dims, kind)


def shift(array, axis, by):
    n = lax.axis_size(axis)
    return lax.ppermute(array, axis, [(i, (i + by) % n) for i in range(n)])


def owner_rows(at, dc, dx):
    t = lax.rem(at[0] + dx, 4) * 2 + (at[1] + dc) % 2
    return pl.ds(pl.multiple_of(t * ROWS, ROWS), ROWS)


def stack(weights, at, shards):
    for shard in shards:
        weights[pl.ds(at, shard.shape[0]), :] = shard[...]
        at += shard.shape[0]


BLOCKS = tuple((dc * 4 + dx, dc, dx) for dc in range(2) for dx in range(4))


def prepare(at, h0, a0, b0, tokens, weights, sems):
    copies = [
        pltpu.make_async_copy(
            h0.at[owner_rows(at, dc, dx), :], tokens.at[b, pl.ds(0, ROWS), :], sems.at[b]
        )
        for b, dc, dx in BLOCKS
    ]
    for copy in copies:
        copy.start()
    stack(weights, 2 * SHARD, (a0, b0))
    for copy in copies:
        copy.wait()


def halve(h1, h3, high, low):
    high[...] = h1[128:, :]
    low[...] = h3[:128, :]


def order_first(at, h1, h3, _, tokens):
    for b, dc, dx in BLOCKS:
        for i, h in ((1, h1), (2, h3)):
            tokens[b, pl.ds(i * ROWS, ROWS), :] = h[owner_rows(at, dc, dx), :]


def order_last(at, h2a, h2b, out):
    for dc in range(2):
        for dx in range(4):
            x = lax.rem(at[0] + dx, 4)
            t = x * 2 + (at[1] + dc) % 2
            rows = pl.ds(pl.multiple_of(lax.rem(t, 4) * ROWS, ROWS), ROWS)

            @pl.when(x < 2)
            def _():
                out[dc * 4 + dx] = h2a[rows, :]

            @pl.when(x >= 2)
            def _():
                out[dc * 4 + dx] = h2b[rows, :]


def lanes_of(j):
    return slice(None) if j is None else pl.ds(pl.multiple_of(j * 256, 256), 256)


def times(tokens, weights, j):
    blocks, rows, _ = tokens.shape
    return (
        lax.dot_general(
            tokens[...].reshape(blocks * rows, K),
            weights[lanes_of(j), :],
            (((1,), (1,)), ((), ())),
            preferred_element_type=jnp.float32,
        )
        .astype(jnp.bfloat16)
        .reshape(blocks, rows, -1)
    )


def store_first(terms, keep, send, j):
    for out, b in ((keep, 0), (send, 4)):
        out[:, pl.ds(0, 2 * ROWS), lanes_of(j)] = terms[b : b + 4, : 2 * ROWS]
        out[:, pl.ds(3 * ROWS, ROWS), lanes_of(j)] = terms[b : b + 4, 2 * ROWS :]


def store_last(terms, keep, send, j):
    for out, b in ((keep, 0), (send, 4)):
        out[:, pl.ds(2 * ROWS, ROWS), lanes_of(j)] = terms[b : b + 4]


def project_first(tokens, *refs):
    *shards, _, out, weights = refs
    stack(weights, 0, shards[:4])
    stack(weights, 3 * SHARD, shards[4:])

    def tile(j, _):
        out[:, :, lanes_of(j)] = times(tokens, weights, j)

    lax.fori_loop(0, NEAR // 256, tile, None)


def project_last(tokens, weights, done, keep, send):
    store_last(times(tokens, weights, None), keep, send, None)
    store_first(done[...], keep, send, None)


def stack_far(l3a, l3b, r3a, r3b, weights):
    stack(weights, 80, (l3a, l3b))
    stack(weights, 80 + 2 * SHARD, (r3a, r3b))


def project_far(first, last, r4a, l4b, _, keep, send, weights):
    stack(weights, 80 + SHARD, (r4a, l4b))

    def tile(j, _):
        store_first(times(first, weights, j), keep, send, j)
        store_last(times(last, weights, j), keep, send, j)

    lax.fori_loop(0, FAR // 256, tile, None)


def pair_sum(keep, other, dx):
    return keep[dx].astype(jnp.float32) + other[dx].astype(jnp.float32)


def add_pair(keep, other, own, s1, s2, s3):
    own[...] = pair_sum(keep, other, 0)
    for dx, out in ((1, s1), (2, s2), (3, s3)):
        out[...] = pair_sum(keep, other, dx).astype(jnp.bfloat16)


def own_rows_of(at, n0, n1, n2, n3, f0, f1, f2, f3, o0, o1, o2, o3, columns):
    def total(parts, lanes):
        return functools.reduce(jnp.add, [p[:, lanes].astype(jnp.float32) for p in parts])

    near_sum = functools.partial(total, (n0, n1, n2, n3))
    far_sum = functools.partial(total, (f0, f1, f2, f3))
    columns[:, :640] = near_sum(slice(0, 640))
    lane = lax.broadcasted_iota(jnp.int32, (128, 128), 1)
    columns[:, 640:768] = jnp.where(
        lane < 80, near_sum(slice(640, 768)), far_sum(slice(0, 128))
    )
    columns[:, 768:] = far_sum(slice(128, 512))
    turn = lax.rem(at[3] + 6, 8) * SHARD
    whole = pltpu.roll(columns[...], turn, 1).astype(jnp.bfloat16)
    for d, out in enumerate((o0, o1, o2, o3)):
        out[...] = whole[d * ROWS : (d + 1) * ROWS, :]


def rms(values, gain_vector):
    return (
        values
        * lax.rsqrt(jnp.mean(values * values, axis=-1, keepdims=True) + norm_epsilon)
        * gain_vector
    )


def finish(at, r0, r1, r2, r3, residual, post_gain, pre_gain, stream_out, peaks, summed):
    for d, block in enumerate((r0, r1, r2, r3)):
        place = lax.rem(at[2] + (4 - d), 4) * 1152
        summed[:, pl.ds(pl.multiple_of(place, 1152), 1152)] = block[...].astype(jnp.float32)
    t = at[0] * 2 + at[1]
    total = summed[...]
    own = residual[pl.ds(pl.multiple_of(t * ROWS, ROWS), ROWS), :]
    stream = own.astype(jnp.float32) + rms(total, post_gain[...])
    stream_out[...] = stream.astype(jnp.bfloat16)
    normed = rms(stream, pre_gain[...])
    most = [
        jnp.max(jnp.abs(v), axis=(0, 1), keepdims=True) for v in (total, stream, normed)
    ]
    column = lax.broadcasted_iota(jnp.int32, (256, 128), 1)
    peaks[...] = jnp.where(column == 0, most[0], jnp.where(column == 1, most[1], most[2]))


def cast_rows(dc, at, scale, pre_gain, *refs):
    blocks, (cast_out, residual_out, cast, sems) = refs[:4], refs[-4:]
    s = scale[0]
    back = 1.0 / jnp.full((1, 1), s, jnp.float32)
    copies = []
    for d, block in enumerate(blocks):
        t = lax.rem(at[0] + (4 - d), 4) * 2 + (at[1] + dc) % 2
        rows = pl.ds(pl.multiple_of(t * ROWS, ROWS), ROWS)
        copies.append(pltpu.make_async_copy(block, residual_out.at[rows, :], sems.at[0, d]))
        copies[-1].start()
        normed = rms(block[...].astype(jnp.float32), pre_gain[...])
        cast[d] = (jnp.clip(normed * s, -float_limit, float_limit) * back).astype(jnp.bfloat16)
        copies.append(pltpu.make_async_copy(cast.at[d], cast_out.at[rows, :], sems.at[1, d]))
        copies[-1].start()
    for copy in copies:
        copy.wait()


def cast(scaled, blocks, dc, halves):
    return call(
        functools.partial(cast_rows, dc),
        [SMEM, SMEM] + [VMEM] * 5 + [ANY] * (2 if halves else 0),
        [shape((256, D)), shape((256, D))],
        [pltpu.VMEM((4, ROWS, D), jnp.bfloat16), pltpu.SemaphoreType.DMA((2, 4))],
        mib=6,
        out=ANY,
        aliases={7: 0, 8: 1} if halves else {},
    )(*scaled, *blocks, *(halves or ()))


def sums_along_x(keep, send):
    other = shift(send, "c", 1)
    width = keep.shape[2]
    own, *others = call(
        add_pair, [VMEM] * 2, [shape((128, width), jnp.float32)] + [shape((128, width))] * 3
    )(keep, other)
    return own, *(shift(s, "x", d) for d, s in enumerate(others, 1))


def on_device(hidden, down_weight, residual, post_gain, pre_gain, cast_scale, amax_history):
    at = jnp.stack([lax.axis_index(a) for a in ("x", "c", "y", "z")]).astype(jnp.int32)
    shards = down_weight.T
    a0, b0 = shards[:80], shards[80:]

    right, left = {0: (a0, b0)}, {0: (a0, b0)}
    for step in (1, 2, 3):
        ar = shift(right[step - 1][0], "z", 1)
        al = shift(left[step - 1][0], "z", -1)
        br = shift(right[step - 1][1], "z", 1)
        bl = shift(left[step - 1][1], "z", -1)
        right[step], left[step] = (ar, br), (al, bl)
    w4 = (shift(right[3][0], "z", 1), shift(left[3][1], "z", -1))

    h3, h1 = shift(hidden, "y", 1), shift(hidden, "y", -1)
    high, low = call(halve, [VMEM] * 2, [shape((128, K))] * 2, mib=5)(h1, h3)
    h2a, h2b = shift(low, "y", 1), shift(high, "y", -1)

    tokens, near_weights = call(
        prepare,
        [SMEM, ANY] + [VMEM] * 2,
        [shape((8, 96, K)), shape((NEAR, K))],
        [pltpu.SemaphoreType.DMA((8,))],
        mib=9,
    )(at, hidden, a0, b0)
    (first,) = call(
        order_first, [SMEM] + [VMEM] * 3, [shape((8, 96, K))], mib=10, aliases={3: 0}
    )(at, h1, h3, tokens)
    (last,) = call(order_last, [SMEM] + [VMEM] * 2, [shape((8, ROWS, K))], mib=4)(at, h2a, h2b)

    near_shards = (*right[2], *right[1], *left[1], *left[2])
    near, near_weights = call(
        project_first,
        [VMEM] * (2 + len(near_shards)),
        [shape((8, 96, NEAR)), shape((NEAR, K))],
        aliases={9: 1},
        mib=14,
    )(first, *near_shards, near_weights)
    keep, send = call(
        project_last, [VMEM] * 3, [shape((4, 128, NEAR))] * 2, mib=9
    )(last, near_weights, near)
    near_parts = sums_along_x(keep, send)

    (far_weights,) = call(stack_far, [VMEM] * 4, [shape((FAR, K))], mib=5)(*left[3], *right[3])
    keep, send, _ = call(
        project_far,
        [VMEM] * 5,
        [shape((4, 128, FAR))] * 2 + [shape((FAR, K))],
        aliases={4: 2},
        mib=13,
    )(first, last, *w4, far_weights)
    far_parts = sums_along_x(keep, send)

    o0, o1, o2, o3 = call(
        own_rows_of,
        [SMEM] + [VMEM] * 8,
        [shape((ROWS, 1152))] * 4,
        [pltpu.VMEM((128, 1152), jnp.float32)],
    )(at, *near_parts, *far_parts)
    r1, r2, r3 = (shift(o, "y", d) for d, o in ((1, o1), (2, o2), (3, o3)))

    stream, peaks = call(
        finish,
        [SMEM] + [VMEM] * 7,
        [shape((ROWS, D)), shape((256, 128), jnp.float32)],
        [pltpu.VMEM((ROWS, D), jnp.float32)],
        mib=8,
    )(at, o0, r1, r2, r3, residual, post_gain[None], pre_gain[None])

    mine = [stream] + [shift(stream, "x", d) for d in (1, 2, 3)]
    partners = [shift(block, "c", 1) for block in mine]

    everyone = lax.all_to_all(
        peaks[:, None], DP + TENSOR, 0, 0, tiled=True
    )
    peak_values = jnp.max(everyone[:, 0, :3], axis=0)

    scaled = (at, cast_scale, pre_gain[None])
    halves = cast(scaled, mine, 0, None)
    cast_out, residual_out = cast(scaled, partners, 1, halves)

    new_history = jnp.concatenate([peak_values[:, None], amax_history[:, :-1]], axis=1)
    new_scales = float_limit / jnp.maximum(jnp.max(new_history, axis=1), 1.0)
    return (cast_out, residual_out, peak_values, new_history, new_scales)


def solution(mesh):
    split = Mesh(mesh.devices.reshape(4, 8, 4, 2), ("y", "z", "x", "c"))
    in_specs = (P(DP, TENSOR), P(TENSOR, DP), P(DP, None), P(), P(), P(), P())
    out_specs = (P(DP, None), P(DP, None), P(), P(), P())

    return jax.shard_map(
        on_device, mesh=split, in_specs=in_specs, out_specs=out_specs, check_vma=False
    )
```

```python
import functools

import jax
import jax.numpy as jnp
from jax import lax
from jax.experimental import pallas as pl
from jax.experimental.pallas import tpu as pltpu
from jax.sharding import Mesh
from jax.sharding import PartitionSpec as P


DP = ("y", "z")
TENSOR = ("x", "c")

norm_epsilon = 1e-06
float_limit = 448.0

D = 4608
K = 2304
SHARD = 144
ROWS = 32
NEAR = 768
FAR = 512
VMEM = pl.BlockSpec(memory_space=pltpu.VMEM)
ANY = pl.BlockSpec(memory_space=pl.ANY)
HBM = pl.BlockSpec(memory_space=pltpu.HBM)
SMEM = pl.BlockSpec(memory_space=pltpu.SMEM)


def call(body, ins, outs, scratch=(), mib=4, out=VMEM, aliases={}):
    return pl.pallas_call(
        body,
        in_specs=list(ins),
        out_specs=[out] * len(outs),
        out_shape=outs,
        scratch_shapes=list(scratch),
        input_output_aliases=aliases,
        compiler_params=pltpu.CompilerParams(vmem_limit_bytes=mib * 2**20),
    )


def shape(dims, kind=jnp.bfloat16):
    return jax.ShapeDtypeStruct(dims, kind)


def shift(array, axis, by):
    n = lax.axis_size(axis)
    return lax.ppermute(array, axis, [(i, (i + by) % n) for i in range(n)])


def owner_rows(at, dc, dx):
    t = lax.rem(at[0] + dx, 4) * 2 + (at[1] + dc) % 2
    return pl.ds(pl.multiple_of(t * ROWS, ROWS), ROWS)


def stack(weights, at, shards):
    for shard in shards:
        weights[pl.ds(at, shard.shape[0]), :] = shard[...]
        at += shard.shape[0]


BLOCKS = tuple((dc * 4 + dx, dc, dx) for dc in range(2) for dx in range(4))


def prepare(at, h0, a0, b0, tokens, weights, sems):
    copies = [
        pltpu.make_async_copy(
            h0.at[owner_rows(at, dc, dx), :], tokens.at[b, pl.ds(0, ROWS), :], sems.at[b]
        )
        for b, dc, dx in BLOCKS
    ]
    for copy in copies:
        copy.start()
    stack(weights, 2 * SHARD, (a0, b0))
    for copy in copies:
        copy.wait()


def cut_weights(whole, a0, b0, sems):
    copies = [
        pltpu.make_async_copy(whole.at[pl.ds(0, 80), :], a0, sems.at[0]),
        pltpu.make_async_copy(whole.at[pl.ds(80, 64), :], b0, sems.at[1]),
    ]
    for copy in copies:
        copy.start()
    for copy in copies:
        copy.wait()


def halve(h1, h3, high, low):
    high[...] = h1[128:, :]
    low[...] = h3[:128, :]


def order_first(at, h1, h3, _, tokens):
    for b, dc, dx in BLOCKS:
        for i, h in ((1, h1), (2, h3)):
            tokens[b, pl.ds(i * ROWS, ROWS), :] = h[owner_rows(at, dc, dx), :]


def order_last(at, h2a, h2b, out):
    for dc in range(2):
        for dx in range(4):
            x = lax.rem(at[0] + dx, 4)
            t = x * 2 + (at[1] + dc) % 2
            rows = pl.ds(pl.multiple_of(lax.rem(t, 4) * ROWS, ROWS), ROWS)

            @pl.when(x < 2)
            def _():
                out[dc * 4 + dx] = h2a[rows, :]

            @pl.when(x >= 2)
            def _():
                out[dc * 4 + dx] = h2b[rows, :]


def times(tokens, weights):
    blocks, rows, _ = tokens.shape
    return (
        lax.dot_general(
            tokens[...].reshape(blocks * rows, K),
            weights[...],
            (((1,), (1,)), ((), ())),
            preferred_element_type=jnp.float32,
        )
        .astype(jnp.bfloat16)
        .reshape(blocks, rows, -1)
    )


def store_first(terms, keep, send):
    for out, b in ((keep, 0), (send, 4)):
        out[:, pl.ds(0, 2 * ROWS), :] = terms[b : b + 4, : 2 * ROWS]
        out[:, pl.ds(3 * ROWS, ROWS), :] = terms[b : b + 4, 2 * ROWS :]


def store_last(terms, keep, send):
    for out, b in ((keep, 0), (send, 4)):
        out[:, pl.ds(2 * ROWS, ROWS), :] = terms[b : b + 4]


def stack_first(r1a, l1b, _, weights):
    stack(weights, SHARD, (r1a,))
    stack(weights, 3 * SHARD + 80, (l1b,))


def project_first(tokens, r2a, r2b, r1b, l1a, l2a, l2b, _, out, weights):
    stack(weights, 0, (r2a, r2b))
    stack(weights, SHARD + 80, (r1b,))
    stack(weights, 3 * SHARD, (l1a,))
    stack(weights, 4 * SHARD, (l2a, l2b))

    def half(i, _):
        some = pl.ds(4 * i, 4)
        out[some] = times(tokens.at[some], weights)

    lax.fori_loop(0, 2, half, None)


def project_last(tokens, weights, done, keep, send):
    store_last(times(tokens, weights), keep, send)
    store_first(done[...], keep, send)


def stack_far(l3a, l3b, r3a, r3b, weights):
    stack(weights, 80, (l3a, l3b))
    stack(weights, 80 + 2 * SHARD, (r3a, r3b))


def project_far(first, last, r4a, l4b, _, keep, send, weights):
    stack(weights, 80 + SHARD, (r4a, l4b))

    store_first(times(first, weights), keep, send)
    store_last(times(last, weights), keep, send)


def pair_sum(keep, other, dx):
    return keep[dx].astype(jnp.float32) + other[dx].astype(jnp.float32)


def add_pair(keep, other, own, s1, s2, s3):
    own[...] = pair_sum(keep, other, 0)
    for dx, out in ((1, s1), (2, s2), (3, s3)):
        out[...] = pair_sum(keep, other, dx).astype(jnp.bfloat16)


def own_rows_of(at, n0, n1, n2, n3, f0, f1, f2, f3, o0, o1, o2, o3, columns):
    def total(parts, lanes):
        return functools.reduce(jnp.add, [p[:, lanes].astype(jnp.float32) for p in parts])

    near_sum = functools.partial(total, (n0, n1, n2, n3))
    far_sum = functools.partial(total, (f0, f1, f2, f3))
    columns[:, :640] = near_sum(slice(0, 640))
    lane = lax.broadcasted_iota(jnp.int32, (128, 128), 1)
    columns[:, 640:768] = jnp.where(
        lane < 80, near_sum(slice(640, 768)), far_sum(slice(0, 128))
    )
    columns[:, 768:] = far_sum(slice(128, 512))
    turn = lax.rem(at[3] + 6, 8) * SHARD
    whole = pltpu.roll(columns[...], turn, 1).astype(jnp.bfloat16)
    for d, out in enumerate((o0, o1, o2, o3)):
        out[...] = whole[d * ROWS : (d + 1) * ROWS, :]


def rms(values, gain_vector):
    return (
        values
        * lax.rsqrt(jnp.mean(values * values, axis=-1, keepdims=True) + norm_epsilon)
        * gain_vector
    )


def finish(at, r0, r1, r2, r3, residual, post_gain, pre_gain, stream_out, peaks, summed):
    for d, block in enumerate((r0, r1, r2, r3)):
        place = lax.rem(at[2] + (4 - d), 4) * 1152
        summed[:, pl.ds(pl.multiple_of(place, 1152), 1152)] = block[...].astype(jnp.float32)
    t = at[0] * 2 + at[1]
    total = summed[...]
    own = residual[pl.ds(pl.multiple_of(t * ROWS, ROWS), ROWS), :]
    stream = own.astype(jnp.float32) + rms(total, post_gain[...])
    stream_out[...] = stream.astype(jnp.bfloat16)
    normed = rms(stream, pre_gain[...])
    most = [
        jnp.max(jnp.abs(v), axis=(0, 1), keepdims=True) for v in (total, stream, normed)
    ]
    column = lax.broadcasted_iota(jnp.int32, (256, 128), 1)
    peaks[...] = jnp.where(column == 0, most[0], jnp.where(column == 1, most[1], most[2]))


def cast_rows(dc, at, scale, pre_gain, *refs):
    blocks, (cast_out, residual_out, cast, sems) = refs[:4], refs[-4:]
    s = scale[0]
    back = 1.0 / jnp.full((1, 1), s, jnp.float32)
    copies = []
    for d, block in enumerate(blocks):
        t = lax.rem(at[0] + (4 - d), 4) * 2 + (at[1] + dc) % 2
        rows = pl.ds(pl.multiple_of(t * ROWS, ROWS), ROWS)
        copies.append(pltpu.make_async_copy(block, residual_out.at[rows, :], sems.at[0, d]))
        copies[-1].start()
        normed = rms(block[...].astype(jnp.float32), pre_gain[...])
        cast[d] = (jnp.clip(normed * s, -float_limit, float_limit) * back).astype(jnp.bfloat16)
        copies.append(pltpu.make_async_copy(cast.at[d], cast_out.at[rows, :], sems.at[1, d]))
        copies[-1].start()
    for copy in copies:
        copy.wait()


def cast(scaled, blocks, dc, halves):
    return call(
        functools.partial(cast_rows, dc),
        [SMEM, SMEM] + [VMEM] * 5 + [ANY] * (2 if halves else 0),
        [shape((256, D)), shape((256, D))],
        [pltpu.VMEM((4, ROWS, D), jnp.bfloat16), pltpu.SemaphoreType.DMA((2, 4))],
        mib=6,
        out=ANY,
        aliases={7: 0, 8: 1} if halves else {},
    )(*scaled, *blocks, *(halves or ()))


def sums_along_x(keep, send):
    other = shift(send, "c", 1)
    width = keep.shape[2]
    own, *others = call(
        add_pair, [VMEM] * 2, [shape((128, width), jnp.float32)] + [shape((128, width))] * 3
    )(keep, other)
    return own, *(shift(s, "x", d) for d, s in enumerate(others, 1))


def on_device(hidden, down_weight, residual, post_gain, pre_gain, cast_scale, amax_history):
    at = jnp.stack([lax.axis_index(a) for a in ("x", "c", "y", "z")]).astype(jnp.int32)
    a0, b0 = call(
        cut_weights, [HBM], [shape((80, K)), shape((64, K))], [pltpu.SemaphoreType.DMA((2,))], mib=2
    )(down_weight.T)

    right, left = {0: (a0, b0)}, {0: (a0, b0)}
    for step in (1, 2, 3):
        ar = shift(right[step - 1][0], "z", 1)
        al = shift(left[step - 1][0], "z", -1)
        br = shift(right[step - 1][1], "z", 1)
        bl = shift(left[step - 1][1], "z", -1)
        right[step], left[step] = (ar, br), (al, bl)
    w4 = (shift(right[3][0], "z", 1), shift(left[3][1], "z", -1))

    h3, h1 = shift(hidden, "y", 1), shift(hidden, "y", -1)
    high, low = call(halve, [VMEM] * 2, [shape((128, K))] * 2, mib=5)(h1, h3)
    h2a, h2b = shift(low, "y", 1), shift(high, "y", -1)

    tokens, near_weights = call(
        prepare,
        [SMEM, HBM] + [VMEM] * 2,
        [shape((8, 96, K)), shape((NEAR, K))],
        [pltpu.SemaphoreType.DMA((8,))],
        mib=9,
    )(at, hidden, a0, b0)
    (first,) = call(
        order_first, [SMEM] + [VMEM] * 3, [shape((8, 96, K))], mib=10, aliases={3: 0}
    )(at, h1, h3, tokens)
    (last,) = call(order_last, [SMEM] + [VMEM] * 2, [shape((8, ROWS, K))], mib=4)(at, h2a, h2b)

    (near_weights,) = call(
        stack_first, [VMEM] * 3, [shape((NEAR, K))], mib=9, aliases={2: 0}
    )(right[1][0], left[1][1], near_weights)
    near_shards = (*right[2], right[1][1], left[1][0], *left[2])
    near, near_weights = call(
        project_first,
        [VMEM] * (2 + len(near_shards)),
        [shape((8, 96, NEAR)), shape((NEAR, K))],
        aliases={7: 1},
        mib=14,
    )(first, *near_shards, near_weights)
    keep, send = call(
        project_last, [VMEM] * 3, [shape((4, 128, NEAR))] * 2, mib=9
    )(last, near_weights, near)
    near_parts = sums_along_x(keep, send)

    (far_weights,) = call(stack_far, [VMEM] * 4, [shape((FAR, K))], mib=5)(*left[3], *right[3])
    keep, send, _ = call(
        project_far,
        [VMEM] * 5,
        [shape((4, 128, FAR))] * 2 + [shape((FAR, K))],
        aliases={4: 2},
        mib=13,
    )(first, last, *w4, far_weights)
    far_parts = sums_along_x(keep, send)

    o0, o1, o2, o3 = call(
        own_rows_of,
        [SMEM] + [VMEM] * 8,
        [shape((ROWS, 1152))] * 4,
        [pltpu.VMEM((128, 1152), jnp.float32)],
    )(at, *near_parts, *far_parts)
    r1, r2, r3 = (shift(o, "y", d) for d, o in ((1, o1), (2, o2), (3, o3)))

    stream, peaks = call(
        finish,
        [SMEM] + [VMEM] * 7,
        [shape((ROWS, D)), shape((256, 128), jnp.float32)],
        [pltpu.VMEM((ROWS, D), jnp.float32)],
        mib=8,
    )(at, o0, r1, r2, r3, residual, post_gain[None], pre_gain[None])

    mine = [stream] + [shift(stream, "x", d) for d in (1, 2, 3)]
    partners = [shift(block, "c", 1) for block in mine]

    everyone = lax.all_to_all(
        peaks[:, None], DP + TENSOR, 0, 0, tiled=True
    )
    peak_values = jnp.max(everyone[:, 0, :3], axis=0)

    scaled = (at, cast_scale, pre_gain[None])
    halves = cast(scaled, mine, 0, None)
    cast_out, residual_out = cast(scaled, partners, 1, halves)

    new_history = jnp.concatenate([peak_values[:, None], amax_history[:, :-1]], axis=1)
    new_scales = float_limit / jnp.maximum(jnp.max(new_history, axis=1), 1.0)
    return (cast_out, residual_out, peak_values, new_history, new_scales)


def solution(mesh):
    split = Mesh(mesh.devices.reshape(4, 8, 4, 2), ("y", "z", "x", "c"))
    in_specs = (P(DP, TENSOR), P(TENSOR, DP), P(DP, None), P(), P(), P(), P())
    out_specs = (P(DP, None), P(DP, None), P(), P(), P())

    return jax.shard_map(
        on_device, mesh=split, in_specs=in_specs, out_specs=out_specs, check_vma=False
    )
```
